128 devices in a mesh: dp: 16 (over z, y), tp: 8 (over x, core).
Axes of the slice: x: 4, y: 4, z: 4, core: 2. Of those that a mesh axis runs over, the one named last changes fastest.
Arguments:
- w_up: bfloat16 [2, 1536, 6144], P(None, None, 'tp')
- w_down: bfloat16 [2, 6144, 1536], P(None, 'tp')
- x_saved: bfloat16 [2, 16, 2048, 1536], P(None, 'dp')
- h_saved: bfloat16 [2, 16, 2048, 6144], P(None, 'dp', None, 'tp')
- grad_out: bfloat16 [16, 2048, 1536], P('dp')
Outputs:
- output 1: bfloat16 [16, 2048, 1536], P('dp')
- output 2: float32 [2, 1536, 6144], P(None, None, 'tp')
- output 3: float32 [2, 6144, 1536], P(None, 'tp')
All inputs are finite; a program needn't handle non-finite values.
Results may differ from the reference program's by a relative error of at most 0.0137507.
Values are sent between devices in bfloat16 or wider.
A program may use at most 1 GiB of HBM per device.

```python
import jax
import jax.numpy as jnp
from jax import lax

LAYER_COUNT = 2
BATCH_ALL = 16
SEQ_LEN = 2048
D = 1536
F = 6144


def gelu_parts(hidden):
    tanh_val = jnp.tanh(0.7978845608028654 * (hidden + 0.044715 * hidden * hidden * hidden))
    gelu_out = 0.5 * hidden * (1.0 + tanh_val)
    gelu_slope = 0.5 * (1.0 + tanh_val) + 0.5 * hidden * (1.0 - tanh_val * tanh_val) * 0.7978845608028654 * (1.0 + 0.134145 * hidden * hidden)
    return gelu_out, gelu_slope


def forward_saved(x_first, w_up, w_down):
    rows_cur = x_first.reshape(BATCH_ALL * SEQ_LEN, D)
    x_list = []
    h_list = []
    for layer_idx in range(LAYER_COUNT):
        hidden = jnp.dot(rows_cur, w_up[layer_idx], preferred_element_type=jnp.float32).astype(jnp.bfloat16)
        gelu_out = gelu_parts(hidden.astype(jnp.float32))[0]
        branch = jnp.dot(gelu_out.astype(jnp.bfloat16), w_down[layer_idx], preferred_element_type=jnp.float32)
        x_list.append(rows_cur)
        h_list.append(hidden)
        rows_cur = (rows_cur.astype(jnp.float32) + branch).astype(jnp.bfloat16)
    x_saved = jnp.stack(x_list).reshape(LAYER_COUNT, BATCH_ALL, SEQ_LEN, D)
    h_saved = jnp.stack(h_list).reshape(LAYER_COUNT, BATCH_ALL, SEQ_LEN, F)
    return x_saved, h_saved


def setup_inputs(seed: int = 0) -> dict:
    root_key = jax.random.key(seed)
    key_x, key_up, key_down, key_grad = jax.random.split(root_key, 4)
    x_first = jax.random.normal(key_x, (BATCH_ALL, SEQ_LEN, D), jnp.float32).astype(jnp.bfloat16)
    w_up = (jax.random.normal(key_up, (LAYER_COUNT, D, F), jnp.float32) * (D ** -0.5)).astype(jnp.bfloat16)
    w_down = (jax.random.normal(key_down, (LAYER_COUNT, F, D), jnp.float32) * (F ** -0.5)).astype(jnp.bfloat16)
    grad_out = jax.random.normal(key_grad, (BATCH_ALL, SEQ_LEN, D), jnp.float32).astype(jnp.bfloat16)
    x_saved, h_saved = forward_saved(x_first, w_up, w_down)
    return {"w_up": w_up, "w_down": w_down, "x_saved": x_saved, "h_saved": h_saved, "grad_out": grad_out}


def reference(w_up, w_down, x_saved, h_saved, grad_out):
    def one_sequence(accums, seq_idx):
        up_acc, down_acc = accums
        grad_cur = grad_out[seq_idx]
        up_new = [None] * LAYER_COUNT
        down_new = [None] * LAYER_COUNT
        for layer_idx in reversed(range(LAYER_COUNT)):
            x_seq = x_saved[layer_idx, seq_idx]
            gelu_out, gelu_slope = gelu_parts(h_saved[layer_idx, seq_idx].astype(jnp.float32))
            act_grad = jnp.dot(grad_cur, w_down[layer_idx].T, preferred_element_type=jnp.float32)
            hid_grad = (act_grad * gelu_slope).astype(jnp.bfloat16)
            part_sum = jnp.dot(hid_grad, w_up[layer_idx].T, preferred_element_type=jnp.float32)
            down_new[layer_idx] = jnp.dot(gelu_out.astype(jnp.bfloat16).T, grad_cur, preferred_element_type=jnp.float32)
            up_new[layer_idx] = jnp.dot(x_seq.T, hid_grad, preferred_element_type=jnp.float32)
            grad_cur = (grad_cur.astype(jnp.float32) + part_sum).astype(jnp.bfloat16)
        return (up_acc + jnp.stack(up_new), down_acc + jnp.stack(down_new)), grad_cur
    zero_acc = (jnp.zeros((LAYER_COUNT, D, F), jnp.float32), jnp.zeros((LAYER_COUNT, F, D), jnp.float32))
    (up_grad, down_grad), grad_in = lax.scan(one_sequence, zero_acc, jnp.arange(BATCH_ALL))
    return grad_in, up_grad, down_grad
```

```python
import jax
import jax.numpy as jnp
from jax import lax
from jax.experimental import pallas as pl
from jax.experimental.pallas import tpu as pltpu
from jax.sharding import PartitionSpec as P

MESH = pl.DeviceIdType.MESH
F32, BF16 = jnp.float32, jnp.bfloat16
T, D, F = 2048, 1536, 768
HALF = T // 2
TOK = HALF // 4
N1, N2 = F // 8, F // 32
RS1, RS2, AG2, AG1 = range(4)
DIRS = ((0, 1), (1, -1))


def gelu_parts(hidden):
    tanh_val = jnp.tanh(0.7978845608028654 * (hidden + 0.044715 * hidden * hidden * hidden))
    gelu_out = 0.5 * hidden * (1.0 + tanh_val)
    gelu_slope = 0.5 * (1.0 + tanh_val) + 0.5 * hidden * (1.0 - tanh_val * tanh_val) * 0.7978845608028654 * (1.0 + 0.134145 * hidden * hidden)
    return gelu_out, gelu_slope


def backward_kernel(wu_hbm, wd_hbm, x_hbm, h_hbm, g_hbm, buf_a, w0, w1, w2, w3,
                    buf_b, pair_in, h_buf, dh_buf, wu_buf, wd_buf, x_tile, ring1, ring2, xring,
                    dp_send, dp_recv, dp_free, x_send, x_recv, x_free, pair_send, pair_recv, pair_free, load_sem, x_sem):
    weight_sums = (w0, w1, w2, w3)
    dp_pos, tp_pos = lax.axis_index("dp"), lax.axis_index("tp")
    core = lax.rem(tp_pos, 2)
    pos = {"x": tp_pos // 2, "y": lax.rem(dp_pos, 4), "z": dp_pos // 4}

    def wrap(value):
        return lax.rem(value + 4, 4)

    def neighbour(axis, step):
        moved = wrap(pos[axis] + step)
        if axis == "x":
            return {"dp": dp_pos, "tp": moved * 2 + core}
        if axis == "y":
            return {"dp": pos["z"] * 4 + moved, "tp": tp_pos}
        return {"dp": moved * 4 + pos["y"], "tp": tp_pos}

    partner = {"dp": dp_pos, "tp": pos["x"] * 2 + 1 - core}

    def load(src, dst, k):
        copy = pltpu.make_async_copy(src, dst, load_sem.at[k])
        copy.start()
        return copy

    load_h = load(h_hbm.at[1, 0], h_buf, 0)
    load_g = load(g_hbm.at[0], buf_a, 1)
    load_wd = load(wd_hbm.at[1], wd_buf, 2)
    load_wu = load(wu_hbm.at[1], wu_buf, 3)

    barrier = pltpu.get_barrier_semaphore()
    for axis in "xyz":
        for _, step in DIRS:
            pl.semaphore_signal(barrier, inc=1, device_id=neighbour(axis, step), device_id_type=MESH)
    pl.semaphore_signal(barrier, inc=1, device_id=partner, device_id_type=MESH)

    copies = {}

    def dp_start(m, stage, colour, di, piece, src, dst, axis):
        k = ((stage * 2 + colour) * 2 + di) * 3 + piece
        copy = pltpu.make_async_remote_copy(src_ref=src, dst_ref=dst, send_sem=dp_send.at[m, k], recv_sem=dp_recv.at[m, k],
                                            device_id=neighbour(axis, DIRS[di][1]), device_id_type=MESH)
        copy.start()
        copies[m, stage, colour, di, piece] = copy

    def level(m, stage, colour):
        first, second = ("y", "z") if colour == 0 else ("z", "y")
        base = colour * (F // 2)
        if stage in (RS1, AG1):
            return first, base, N1, ring1.at[m % 2, colour]
        return second, base + pos[first] * N1, N2, ring2.at[m % 2, colour]

    def rows(base, j, n):
        return pl.ds(pl.multiple_of(base + j * n, 8), n)

    def rs_start(m, stage):
        w = weight_sums[m]
        for piece in range(2):
            for colour in range(2):
                axis, base, n, ring = level(m, stage, colour)
                for di, step in DIRS:
                    if piece == 0:
                        src = w.at[di, rows(base, wrap(pos[axis] + 2), n)]
                    else:
                        src = w.at[1 - di, rows(base, wrap(pos[axis] + step), n)]
                    dp_start(m, stage, colour, di, piece, src, ring.at[di, piece], axis)

    def rs_mid(m, stage):
        w = weight_sums[m]
        for colour in range(2):
            axis, base, n, ring = level(m, stage, colour)
            for di, step in DIRS:
                copies[m, stage, colour, di, 0].wait_recv()
                near = rows(base, wrap(pos[axis] + step), n)
                w[di, near, :] = w[di, near, :] + ring[di, 0]
                dp_start(m, stage, colour, di, 2, w.at[di, near], ring.at[di, 2], axis)

    def rs_end(m, stage):
        w = weight_sums[m]
        for colour in range(2):
            axis, base, n, ring = level(m, stage, colour)
            for di, _ in DIRS:
                copies[m, stage, colour, di, 1].wait_recv()
                copies[m, stage, colour, di, 2].wait_recv()
            own = rows(base, pos[axis], n)
            for di, _ in DIRS:
                w[di, own, :] = w[di, own, :] + ring[di, 2] + ring[1 - di, 1]
            for di, step in DIRS:
                for piece in range(3):
                    copies[m, stage, colour, di, piece].wait_send()
            for di, step in DIRS:
                pl.semaphore_signal(dp_free.at[m, stage, colour, di], inc=1, device_id=neighbour(axis, -step), device_id_type=MESH)

    def ag_start(m, stage):
        w = weight_sums[m]
        for piece in range(2):
            for colour in range(2):
                axis, base, n, _ = level(m, stage, colour)
                own = rows(base, pos[axis], n)
                for di, _ in DIRS:
                    if piece == 0:
                        pl.semaphore_wait(dp_free.at[m, RS2 if stage == AG2 else RS1, colour, di], 1)
                    part = w.at[di if piece == 0 else 1 - di, own]
                    dp_start(m, stage, colour, di, piece, part, part, axis)

    def ag_mid(m, stage):
        w = weight_sums[m]
        for colour in range(2):
            axis, base, n, _ = level(m, stage, colour)
            for di, step in DIRS:
                copies[m, stage, colour, di, 0].wait_recv()
                part = w.at[di, rows(base, wrap(pos[axis] - step), n)]
                dp_start(m, stage, colour, di, 2, part, part, axis)

    def ag_end(m, stage):
        for colour in range(2):
            for di, _ in DIRS:
                copies[m, stage, colour, di, 1].wait_recv()
                copies[m, stage, colour, di, 2].wait_recv()

    def dp_step(m, k):
        if k == 0:
            rs_start(m, RS1)
        elif k == 1:
            rs_mid(m, RS1)
        elif k == 2:
            rs_end(m, RS1)
            rs_start(m, RS2)
        elif k == 3:
            rs_mid(m, RS2)
        elif k == 4:
            rs_end(m, RS2)
            ag_start(m, AG2)
        elif k == 5:
            ag_mid(m, AG2)
        elif k == 6:
            ag_end(m, AG2)
            ag_start(m, AG1)
        elif k == 7:
            ag_mid(m, AG1)
        else:
            ag_end(m, AG1)
            for key, copy in copies.items():
                if key[0] == m and key[1] in (AG2, AG1):
                    copy.wait_send()

    x_copies, pair_copies = {}, {}

    def x_copy(layer, stage, di, piece, src, dst):
        k = (stage * 2 + di) * 3 + piece
        copy = pltpu.make_async_remote_copy(src_ref=src, dst_ref=dst, send_sem=x_send.at[layer, k], recv_sem=x_recv.at[layer, k],
                                            device_id=neighbour("x", DIRS[di][1]), device_id_type=MESH)
        x_copies[layer, stage, di, piece] = copy
        return copy

    def pair_copy(layer, k, src, dst):
        return pltpu.make_async_remote_copy(src_ref=src, dst_ref=dst, send_sem=pair_send.at[layer, k], recv_sem=pair_recv.at[layer, k],
                                            device_id=partner, device_id_type=MESH)

    def chunk(j, half=None):
        base = core * HALF + j * TOK
        if half is None:
            return pl.ds(pl.multiple_of(base, TOK), TOK)
        return pl.ds(pl.multiple_of(base + half * (TOK // 2), TOK // 2), TOK // 2)

    def block(g_buf, p_buf, row, keep_gelu):
        toks = pl.ds(pl.multiple_of(row, TOK), TOK)
        act_grad = lax.dot_general(g_buf[toks, :], wd_buf[...], (((1,), (1,)), ((), ())), preferred_element_type=F32)
        gelu_out, gelu_slope = gelu_parts(h_buf[toks, :].astype(F32))
        hid_grad = (act_grad * gelu_slope).astype(BF16)
        dh_buf[toks, :] = hid_grad
        if keep_gelu:
            h_buf[toks, :] = gelu_out.astype(BF16)
        p_buf[toks, :] = lax.dot_general(hid_grad, wu_buf[...], (((1,), (1,)), ((), ())), preferred_element_type=F32).astype(BF16)

    def hidden_grads(layer, g_buf, p_buf, keep_gelu):
        for di, step in DIRS:
            far, near = wrap(pos["x"] + 2), wrap(pos["x"] + step)
            x_copy(layer, 0, di, 0, p_buf.at[chunk(far, di)], xring.at[di, 0])
            x_copy(layer, 0, di, 1, p_buf.at[chunk(near, 1 - di)], xring.at[di, 1])

        @pl.loop(0, 4)
        def _(i):
            j = lax.rem(pos["x"] + 2 + i, 4)
            other = pl.multiple_of((1 - core) * HALF + j * TOK, TOK)
            block(g_buf, p_buf, other, keep_gelu)
            landing = pair_in.at[pl.ds(pl.multiple_of(j * TOK, TOK), TOK)]
            copy = pair_copy(layer, i, p_buf.at[pl.ds(other, TOK)], landing)
            copy.start()
            block(g_buf, p_buf, pl.multiple_of(core * HALF + j * TOK, TOK), keep_gelu)
            copy.wait()
            p_buf[chunk(j), :] = (p_buf[chunk(j), :].astype(F32) + landing[...].astype(F32)).astype(BF16)

            @pl.when(i == 0)
            def _():
                for di, _ in DIRS:
                    x_copies[layer, 0, di, 0].start()

            @pl.when(i == 1)
            def _():
                x_copies[layer, 0, 1, 1].start()

            @pl.when(i == 3)
            def _():
                x_copies[layer, 0, 0, 1].start()

        pl.semaphore_signal(pair_free.at[layer], inc=1, device_id=partner, device_id_type=MESH)

    def tp_step(layer, k, g_buf, p_buf):
        if k == 0:
            for di, step in DIRS:
                x_copies[layer, 0, di, 0].wait_recv()
                near = chunk(wrap(pos["x"] + step), di)
                p_buf[near, :] = (p_buf[near, :].astype(F32) + xring[di, 0].astype(F32)).astype(BF16)
                x_copy(layer, 0, di, 2, p_buf.at[near], xring.at[di, 2]).start()
        elif k == 1:
            for di, _ in DIRS:
                x_copies[layer, 0, di, 1].wait_recv()
                x_copies[layer, 0, di, 2].wait_recv()
            for di, step in DIRS:
                for piece in range(3):
                    x_copies[layer, 0, di, piece].wait_send()
            for di, step in DIRS:
                pl.semaphore_signal(x_free.at[layer, di], inc=1, device_id=neighbour("x", -step), device_id_type=MESH)
            for di, _ in DIRS:
                own = chunk(pos["x"], di)
                total = p_buf[own, :].astype(F32) + xring[di, 2].astype(F32) + xring[1 - di, 1].astype(F32)
                p_buf[own, :] = (g_buf[own, :].astype(F32) + total).astype(BF16)
            for piece in range(2):
                for di, _ in DIRS:
                    if piece == 0:
                        pl.semaphore_wait(x_free.at[layer, di], 1)
                    part = p_buf.at[chunk(pos["x"], di if piece == 0 else 1 - di)]
                    x_copy(layer, 1, di, piece, part, part).start()
            pl.semaphore_wait(pair_free.at[layer], 1)
            tp_forward(layer, 0, p_buf, pos["x"])
        elif k == 2:
            for di, step in DIRS:
                x_copies[layer, 1, di, 0].wait_recv()
                part = p_buf.at[chunk(wrap(pos["x"] - step), di)]
                x_copy(layer, 1, di, 2, part, part).start()
        elif k == 3:
            for di, step in DIRS:
                x_copies[layer, 1, di, 1].wait_recv()
                tp_forward(layer, 1 + di, p_buf, wrap(pos["x"] - step))
        elif k == 4:
            for di, _ in DIRS:
                x_copies[layer, 1, di, 2].wait_recv()
            tp_forward(layer, 3, p_buf, wrap(pos["x"] + 2))
        else:
            for k in range(4):
                pair_copies[layer, k].wait()
            for key, copy in x_copies.items():
                if key[:2] == (layer, 1):
                    copy.wait_send()

    def tp_forward(layer, k, p_buf, j):
        part = p_buf.at[chunk(j)]
        copy = pair_copy(layer, 4 + k, part, part)
        copy.start()
        pair_copies[layer, k] = copy

    def down_grad(m, gelu_buf, g_buf):
        w = weight_sums[m]

        @pl.loop(0, F // 256)
        def _(i):
            at = pl.ds(pl.multiple_of(i * 256, 256), 256)
            for half in range(2):
                w[half, at, :] = lax.dot_general(gelu_buf[:, at], g_buf[:, half * F:(half + 1) * F], (((0,), (0,)), ((), ())), preferred_element_type=F32)

    def x_load(layer, i):
        return pltpu.make_async_copy(x_hbm.at[layer, 0, :, pl.ds(pl.multiple_of(i * 256, 256), 256)], x_tile.at[lax.rem(i, 2)], x_sem.at[lax.rem(i, 2)])

    def up_grad_begin(layer):
        x_load(layer, 0).start()
        x_load(layer, 1).start()

    def up_grad(m, layer):
        w = weight_sums[m]

        @pl.loop(0, D // 256)
        def _(i):
            x_load(layer, i).wait()
            w[i // 3, pl.ds(pl.multiple_of(lax.rem(i, 3) * 256, 256), 256), :] = lax.dot_general(
                x_tile[lax.rem(i, 2)], dh_buf[...], (((0,), (0,)), ((), ())), preferred_element_type=F32)

            @pl.when(i + 2 < D // 256)
            def _():
                x_load(layer, i + 2).start()

    up_grad_begin(1)
    load_h.wait()

    @pl.loop(0, T // 256)
    def _(i):
        toks = pl.ds(pl.multiple_of(i * 256, 256), 256)
        dh_buf[toks, :] = gelu_parts(h_buf[toks, :].astype(F32))[0].astype(BF16)

    load_g.wait()
    down_grad(0, dh_buf, buf_a)
    pl.semaphore_wait(barrier, 7)
    dp_step(0, 0)
    load_wd.wait()
    load_wu.wait()
    hidden_grads(1, buf_a, buf_b, False)
    dp_step(0, 1)
    tp_step(1, 0, buf_a, buf_b)
    load_h = load(h_hbm.at[0, 0], h_buf, 0)
    load_wd = load(wd_hbm.at[0], wd_buf, 2)
    load_wu = load(wu_hbm.at[0], wu_buf, 3)
    up_grad(1, 1)
    up_grad_begin(0)
    dp_step(0, 2)
    dp_step(1, 0)
    dp_step(0, 3)
    tp_step(1, 1, buf_a, buf_b)
    dp_step(1, 1)
    dp_step(0, 4)
    tp_step(1, 2, buf_a, buf_b)
    dp_step(1, 2)
    dp_step(0, 5)
    tp_step(1, 3, buf_a, buf_b)
    dp_step(1, 3)
    dp_step(0, 6)
    dp_step(1, 4)
    tp_step(1, 4, buf_a, buf_b)
    dp_step(1, 5)
    tp_step(1, 5, buf_a, buf_b)
    load_h.wait()
    load_wd.wait()
    load_wu.wait()
    dp_step(0, 7)
    dp_step(1, 6)
    hidden_grads(0, buf_b, buf_a, True)
    dp_step(1, 7)
    tp_step(0, 0, buf_b, buf_a)
    down_grad(2, h_buf, buf_b)
    dp_step(0, 8)
    dp_step(2, 0)
    up_grad(3, 0)
    dp_step(1, 8)
    dp_step(2, 1)
    dp_step(3, 0)
    tp_step(0, 1, buf_b, buf_a)
    dp_step(2, 2)
    dp_step(3, 1)
    dp_step(2, 3)
    tp_step(0, 2, buf_b, buf_a)
    dp_step(3, 2)
    dp_step(2, 4)
    dp_step(3, 3)
    tp_step(0, 3, buf_b, buf_a)
    dp_step(2, 5)
    dp_step(3, 4)
    dp_step(2, 6)
    tp_step(0, 4, buf_b, buf_a)
    dp_step(3, 5)
    dp_step(2, 7)
    dp_step(3, 6)
    tp_step(0, 5, buf_b, buf_a)
    dp_step(3, 7)
    dp_step(2, 8)
    dp_step(3, 8)


def flush_kernel(g, w0, w1, w2, w3, g_out, up_out, down_out, sems):
    copies = [pltpu.make_async_copy(g, g_out.at[0], sems.at[0])]
    for layer, (down, up) in ((1, (w0, w1)), (0, (w2, w3))):
        for half in range(2):
            copies.append(pltpu.make_async_copy(up.at[half], up_out.at[layer, pl.ds(half * F, F)], sems.at[len(copies)]))
            copies.append(pltpu.make_async_copy(down.at[half], down_out.at[layer, :, pl.ds(half * F, F)], sems.at[len(copies)]))
    for copy in copies:
        copy.start()
    for copy in copies:
        copy.wait()


def solution(mesh):
    hbm, vmem = pl.BlockSpec(memory_space=pl.ANY), pl.BlockSpec(memory_space=pltpu.VMEM)

    def run_backward(w_up, w_down, x_saved, h_saved, grad_out):
        parts = pl.pallas_call(
            backward_kernel,
            name="backward",
            out_shape=[pltpu.VMEM((T, D), BF16)] + [pltpu.VMEM((2, F, F), F32)] * 4,
            in_specs=[hbm] * 5,
            out_specs=[vmem] * 5,
            scratch_shapes=[
                pltpu.VMEM((T, D), BF16),
                pltpu.VMEM((HALF, D), BF16),
                pltpu.VMEM((T, F), BF16),
                pltpu.VMEM((T, F), BF16),
                pltpu.VMEM((D, F), BF16),
                pltpu.VMEM((F, D), BF16),
                pltpu.VMEM((2, T, 256), BF16),
                pltpu.VMEM((2, 2, 2, 3, N1, F), F32),
                pltpu.VMEM((2, 2, 2, 3, N2, F), F32),
                pltpu.VMEM((2, 3, TOK // 2, D), BF16),
                pltpu.SemaphoreType.DMA((4, 48)),
                pltpu.SemaphoreType.DMA((4, 48)),
                pltpu.SemaphoreType.REGULAR((4, 2, 2, 2)),
                pltpu.SemaphoreType.DMA((2, 12)),
                pltpu.SemaphoreType.DMA((2, 12)),
                pltpu.SemaphoreType.REGULAR((2, 2)),
                pltpu.SemaphoreType.DMA((2, 8)),
                pltpu.SemaphoreType.DMA((2, 8)),
                pltpu.SemaphoreType.REGULAR((2,)),
                pltpu.SemaphoreType.DMA((4,)),
                pltpu.SemaphoreType.DMA((2,)),
            ],
            compiler_params=pltpu.CompilerParams(collective_id=0, has_side_effects=True, vmem_limit_bytes=41800000),
        )(w_up, w_down, x_saved, h_saved, grad_out)
        grad_in, up_total, down_total = pl.pallas_call(
            flush_kernel,
            name="flush",
            out_shape=[jax.ShapeDtypeStruct((1, T, D), BF16), jax.ShapeDtypeStruct((2, D, F), F32), jax.ShapeDtypeStruct((2, F, D), F32)],
            in_specs=[vmem] * 5,
            out_specs=[hbm] * 3,
            scratch_shapes=[pltpu.SemaphoreType.DMA((9,))],
            compiler_params=pltpu.CompilerParams(vmem_limit_bytes=1 << 20),
        )(*parts)
        return grad_in, up_total, down_total

    return jax.shard_map(run_backward, mesh=mesh, in_specs=(P(None, None, "tp"), P(None, "tp", None), P(None, "dp", None, None), P(None, "dp", None, "tp"), P("dp", None, None)), out_specs=(P("dp", None, None), P(None, None, "tp"), P(None, "tp", None)), check_vma=False)
```

```python
import jax
import jax.numpy as jnp
from jax import lax
from jax.experimental import pallas as pl
from jax.experimental.pallas import tpu as pltpu
from jax.sharding import PartitionSpec as P

MESH = pl.DeviceIdType.MESH
F32, BF16 = jnp.float32, jnp.bfloat16
T, D, F = 2048, 1536, 768
HALF = T // 2
TOK = HALF // 4
Q = F // 2
N1, N2 = F // 8, F // 32
PARTS = 8
SLOTS = 4
RS1, RS2, AG2, AG1 = range(4)
DIRS = ((0, 1), (1, -1))

ORDER = (
    "DbaaDddcHHbbacHdcHabUfeeTdUfcgaebfhhdggcTehbfecdabghfecdahgT",
    "bfdechTfagbbaheccTddfTHHbaegfhheHHaDjgighUDjjhfdiillUpjTgicp",
    "kjemmkpjifnlkipnjmnTpgoikljpmnipkjlomknTolpnkmiojnlimkTopnjm",
    "kopmmolloklnTnookolTpnim",
)


def gelu_parts(hidden):
    tanh_val = jnp.tanh(0.7978845608028654 * (hidden + 0.044715 * hidden * hidden * hidden))
    gelu_out = 0.5 * hidden * (1.0 + tanh_val)
    gelu_slope = 0.5 * (1.0 + tanh_val) + 0.5 * hidden * (1.0 - tanh_val * tanh_val) * 0.7978845608028654 * (1.0 + 0.134145 * hidden * hidden)
    return gelu_out, gelu_slope


def backward_kernel(wu_hbm, wd_hbm, x_hbm, h_hbm, g_hbm, buf_a, *refs):
    sums = refs[:PARTS]
    (buf_b, pair_in, h_buf, dh_buf, wu_buf, wd_buf, x_tile, ring1, ring2, xring,
     dp_send, dp_recv, dp_free, x_send, x_recv, x_free, pair_send, pair_recv, pair_free, load_sem, x_sem) = refs[PARTS:]
    dp_pos, tp_pos = lax.axis_index("dp"), lax.axis_index("tp")
    core = lax.rem(tp_pos, 2)
    pos = {"x": tp_pos // 2, "y": lax.rem(dp_pos, 4), "z": dp_pos // 4}
    g_of, p_of = {1: buf_a, 0: buf_b}, {1: buf_b, 0: buf_a}

    def wrap(value):
        return lax.rem(value + 4, 4)

    def neighbour(axis, step):
        moved = wrap(pos[axis] + step)
        if axis == "x":
            return {"dp": dp_pos, "tp": moved * 2 + core}
        if axis == "y":
            return {"dp": pos["z"] * 4 + moved, "tp": tp_pos}
        return {"dp": moved * 4 + pos["y"], "tp": tp_pos}

    partner = {"dp": dp_pos, "tp": pos["x"] * 2 + 1 - core}

    def load(src, dst, k):
        copy = pltpu.make_async_copy(src, dst, load_sem.at[k])
        copy.start()
        return copy

    def x_load(layer, i):
        slot = lax.rem(i, 2)
        return pltpu.make_async_copy(x_hbm.at[layer, 0, :, pl.ds(pl.multiple_of(i * 256, 256), 256)], x_tile.at[slot], x_sem.at[slot])

    h_rows = [pl.ds(i * (T // 4), T // 4) for i in range(4)]
    load_h = [load(h_hbm.at[1, 0, h_rows[i]], h_buf.at[h_rows[i]], i) for i in range(4)]
    load_g = [load(g_hbm.at[0, :, pl.ds(i * F, F)], buf_a.at[:, pl.ds(i * F, F)], 4 + i) for i in range(2)]
    load_w = [load(wd_hbm.at[1], wd_buf, 6), load(wu_hbm.at[1], wu_buf, 7)]
    x_load(1, 0).start()
    x_load(1, 1).start()

    barrier = pltpu.get_barrier_semaphore()
    for axis in "xyz":
        for _, step in DIRS:
            pl.semaphore_signal(barrier, inc=1, device_id=neighbour(axis, step), device_id_type=MESH)
    pl.semaphore_signal(barrier, inc=1, device_id=partner, device_id_type=MESH)

    def remote(src, dst, send_sem, recv_sem, device):
        return pltpu.make_async_remote_copy(src_ref=src, dst_ref=dst, send_sem=send_sem, recv_sem=recv_sem, device_id=device, device_id_type=MESH)

    def dp_axes(stage, colour):
        first, second = ("y", "z") if colour == 0 else ("z", "y")
        return first if stage in (RS1, AG1) else second

    def dp_rows(stage, colour, j):
        if stage in (RS1, AG1):
            return pl.ds(pl.multiple_of(colour * (F // 2) + j * N1, 8), N1)
        return pl.ds(pl.multiple_of(colour * (F // 2) + pos[dp_axes(RS1, colour)] * N1 + j * N2, 8), N2)

    def dp_ring(n, stage, colour):
        return (ring1 if stage in (RS1, AG1) else ring2).at[n % SLOTS, colour]

    def dp_copy(n, stage, colour, di, piece):
        w, axis, step = sums[n], dp_axes(stage, colour), DIRS[di][1]
        p = pos[axis]
        if stage in (RS1, RS2):
            dst = dp_ring(n, stage, colour).at[di, piece]
            if piece == 0:
                src = w.at[di, dp_rows(stage, colour, wrap(p + 2))]
            else:
                src = w.at[1 - di if piece == 1 else di, dp_rows(stage, colour, wrap(p + step))]
        else:
            j = p if piece < 2 else wrap(p - step)
            src = dst = w.at[1 - di if piece == 1 else di, dp_rows(stage, colour, j)]
        return remote(src, dst, dp_send.at[n % SLOTS, stage, colour], dp_recv.at[n % SLOTS, stage, colour, min(piece, 1)], neighbour(axis, step))

    def dp_received(n, stage, colour, last):
        ring = dp_ring(n, stage, colour)
        pieces = ring.at[:, pl.ds(1, 2)] if last else ring.at[:, pl.ds(0, 1)]
        remote(pieces, pieces, dp_send.at[n % SLOTS, stage, colour], dp_recv.at[n % SLOTS, stage, colour, last], partner).wait_recv()

    def dp_sent(n, stage, colour):
        ring = dp_ring(n, stage, colour)
        remote(ring, ring, dp_send.at[n % SLOTS, stage, colour], dp_recv.at[n % SLOTS, stage, colour, 0], partner).wait_send()

    def both(n, stage, colour, piece):
        for di, _ in DIRS:
            dp_copy(n, stage, colour, di, piece).start()

    def rs_mid(n, stage, colour):
        w, axis, ring = sums[n], dp_axes(stage, colour), dp_ring(n, stage, colour)
        dp_received(n, stage, colour, 0)
        for di, step in DIRS:
            near = dp_rows(stage, colour, wrap(pos[axis] + step))
            w[di, near, :] = w[di, near, :] + ring[di, 0]
            dp_copy(n, stage, colour, di, 2).start()

    def rs_end(n, stage, colour):
        w, axis, ring = sums[n], dp_axes(stage, colour), dp_ring(n, stage, colour)
        dp_received(n, stage, colour, 1)
        own = dp_rows(stage, colour, pos[axis])
        for di, _ in DIRS:
            w[di, own, :] = w[di, own, :] + ring[di, 2] + ring[1 - di, 1]

    def rs_free(n, stage, colour):
        dp_sent(n, stage, colour)
        for _, step in DIRS:
            pl.semaphore_signal(dp_free.at[n, stage, colour], inc=1, device_id=neighbour(dp_axes(stage, colour), step), device_id_type=MESH)

    def ag_ready(n, stage, colour):
        pl.semaphore_wait(dp_free.at[n, RS2 if stage == AG2 else RS1, colour], 2)

    def ag_mid(n, stage, colour):
        dp_received(n, stage, colour, 0)
        both(n, stage, colour, 2)

    def dp_step(n, colour, k):
        if k < 2:
            both(n, RS1, colour, k)
        elif k == 2:
            rs_mid(n, RS1, colour)
        elif k == 3:
            rs_end(n, RS1, colour)
            both(n, RS2, colour, 0)
            both(n, RS2, colour, 1)
            rs_free(n, RS1, colour)
        elif k == 4:
            rs_mid(n, RS2, colour)
        elif k == 5:
            rs_end(n, RS2, colour)
            rs_free(n, RS2, colour)
            ag_ready(n, AG2, colour)
            both(n, AG2, colour, 0)
            both(n, AG2, colour, 1)
        elif k == 6:
            ag_mid(n, AG2, colour)
        elif k == 7:
            dp_received(n, AG2, colour, 1)
            ag_ready(n, AG1, colour)
            both(n, AG1, colour, 0)
        elif k == 8:
            both(n, AG1, colour, 1)
        elif k == 9:
            ag_mid(n, AG1, colour)
        else:
            dp_received(n, AG1, colour, 1)
            dp_sent(n, AG2, colour)
            dp_sent(n, AG1, colour)

    def chunk(j, half=None):
        base = core * HALF + j * TOK
        if half is None:
            return pl.ds(pl.multiple_of(base, TOK), TOK)
        return pl.ds(pl.multiple_of(base + half * (TOK // 2), TOK // 2), TOK // 2)

    def x_copy(layer, stage, di, piece):
        p_buf, step, p = p_of[layer], DIRS[di][1], pos["x"]
        if stage == 0:
            dst = xring.at[di, piece]
            src = p_buf.at[chunk(wrap(p + 2), di) if piece == 0 else chunk(wrap(p + step), 1 - di if piece == 1 else di)]
        else:
            src = dst = p_buf.at[chunk(p if piece < 2 else wrap(p - step), 1 - di if piece == 1 else di)]
        recv = min(piece, 1) if stage == 0 else 2 + piece
        return remote(src, dst, x_send.at[layer, stage], x_recv.at[layer, recv], neighbour("x", step))

    def x_received(layer, recv):
        pieces = xring.at[:, pl.ds(1, 2)] if recv == 1 else xring.at[:, pl.ds(0, 1)]
        remote(pieces, pieces, x_send.at[layer, 0], x_recv.at[layer, recv], partner).wait_recv()

    def x_sent(layer, stage):
        remote(xring, xring, x_send.at[layer, stage], x_recv.at[layer, 0], partner).wait_send()

    def pair_copy(layer, k, src, dst):
        return remote(src, dst, pair_send.at[layer, k], pair_recv.at[layer, k], partner)

    def tp_forward(layer, k):
        part = p_of[layer].at[chunk(wrap(pos["x"] + (0, -1, 1, 2)[k]))]
        return pair_copy(layer, 4, part, part)

    def block(layer, row):
        toks = pl.ds(pl.multiple_of(row, TOK), TOK)
        act_grad = lax.dot_general(g_of[layer][toks, :], wd_buf[...], (((1,), (1,)), ((), ())), preferred_element_type=F32)
        gelu_out, gelu_slope = gelu_parts(h_buf[toks, :].astype(F32))
        hid_grad = (act_grad * gelu_slope).astype(BF16)
        dh_buf[toks, :] = hid_grad
        if layer == 0:
            h_buf[toks, :] = gelu_out.astype(BF16)
        p_of[layer][toks, :] = lax.dot_general(hid_grad, wu_buf[...], (((1,), (1,)), ((), ())), preferred_element_type=F32).astype(BF16)

    def hidden_grads(layer, hooks):
        p_buf = p_of[layer]

        @pl.loop(0, 4)
        def _(i):
            j = lax.rem(pos["x"] + 2 + i, 4)
            other = pl.multiple_of((1 - core) * HALF + j * TOK, TOK)
            block(layer, other)
            landing = pair_in.at[pl.ds(pl.multiple_of(j * TOK, TOK), TOK)]
            copy = pair_copy(layer, i, p_buf.at[pl.ds(other, TOK)], landing)
            copy.start()
            block(layer, pl.multiple_of(core * HALF + j * TOK, TOK))
            copy.wait()
            p_buf[chunk(j), :] = (p_buf[chunk(j), :].astype(F32) + landing[...].astype(F32)).astype(BF16)
            for k in range(4):

                @pl.when(i == k)
                def _():
                    if k == 0:
                        x_copy(layer, 0, 0, 0).start()
                        x_copy(layer, 0, 1, 0).start()
                    elif k == 1:
                        x_copy(layer, 0, 1, 1).start()
                    elif k == 3:
                        x_copy(layer, 0, 0, 1).start()
                        pl.semaphore_signal(pair_free.at[layer], inc=1, device_id=partner, device_id_type=MESH)
                    for op in hooks[k]:
                        run(op)

    def tp_step(layer, k):
        g_buf, p_buf = g_of[layer], p_of[layer]
        if k == 0:
            x_received(layer, 0)
            for di, step in DIRS:
                near = chunk(wrap(pos["x"] + step), di)
                p_buf[near, :] = (p_buf[near, :].astype(F32) + xring[di, 0].astype(F32)).astype(BF16)
                x_copy(layer, 0, di, 2).start()
        elif k == 1:
            x_received(layer, 1)
            x_sent(layer, 0)
            for _, step in DIRS:
                pl.semaphore_signal(x_free.at[layer], inc=1, device_id=neighbour("x", step), device_id_type=MESH)
            for di, _ in DIRS:
                own = chunk(pos["x"], di)
                total = p_buf[own, :].astype(F32) + xring[di, 2].astype(F32) + xring[1 - di, 1].astype(F32)
                p_buf[own, :] = (g_buf[own, :].astype(F32) + total).astype(BF16)
            pl.semaphore_wait(x_free.at[layer], 2)
            for piece in range(2):
                for di, _ in DIRS:
                    x_copy(layer, 1, di, piece).start()
            pl.semaphore_wait(pair_free.at[layer], 1)
            tp_forward(layer, 0).start()
        elif k == 2:
            x_received(layer, 2)
            for di, _ in DIRS:
                x_copy(layer, 1, di, 2).start()
        elif k == 3:
            x_received(layer, 3)
            tp_forward(layer, 1).start()
            tp_forward(layer, 2).start()
        elif k == 4:
            x_received(layer, 4)
            tp_forward(layer, 3).start()
        else:
            pair_copy(layer, 4, pair_in, pair_in).wait()
            x_sent(layer, 1)

    def put(w, at, value):
        w[0, at, :] = value[:, :Q]
        w[1, at, :] = value[:, Q:]

    def down_grad(layer, half):
        gelu_buf, g_buf = (dh_buf, buf_a) if layer == 1 else (h_buf, buf_b)

        @pl.loop(0, F // 256)
        def _(i):
            at = pl.ds(pl.multiple_of(i * 256, 256), 256)
            put(sums[(1 - layer) * 4 + half], at,
                lax.dot_general(gelu_buf[:, at], g_buf[:, half * F:(half + 1) * F], (((0,), (0,)), ((), ())), preferred_element_type=F32))

    def up_grad(layer, half):
        @pl.loop(0, F // 256)
        def _(t):
            i = half * (F // 256) + t
            x_load(layer, i).wait()
            put(sums[(1 - layer) * 4 + 2 + half], pl.ds(pl.multiple_of(t * 256, 256), 256),
                lax.dot_general(x_tile[lax.rem(i, 2)], dh_buf[...], (((0,), (0,)), ((), ())), preferred_element_type=F32))

            @pl.when(i + 2 < D // 256)
            def _():
                x_load(layer, i + 2).start()

        if layer == 1 and half == 1:
            x_load(0, 0).start()
            x_load(0, 1).start()

    taken = {}

    def run(letter):
        count = taken[letter] = taken.get(letter, -1) + 1
        if letter == "D":
            down_grad(1 - count // 2, count % 2)
        elif letter == "U":
            up_grad(1 - count // 2, count % 2)
        elif letter == "T":
            tp_step(1 - count // 6, count % 6)
        else:
            part = ord(letter) - ord("a")
            dp_step(part // 2, part % 2, count)

    for i in range(4):
        load_h[i].wait()

        @pl.loop(2 * i, 2 * i + 2)
        def _(b):
            toks = pl.ds(pl.multiple_of(b * 256, 256), 256)
            dh_buf[toks, :] = gelu_parts(h_buf[toks, :].astype(F32))[0].astype(BF16)

    todo = list("".join(ORDER))
    layer = 1
    for half in range(2):
        load_g[half].wait()
        while todo[0] != "D":
            run(todo.pop(0))
        run(todo.pop(0))
        if half == 0:
            pl.semaphore_wait(barrier, 7)
    while todo:
        if todo[0] != "H":
            run(todo.pop(0))
            continue
        hooks = []
        while len(hooks) < 4:
            letter = todo.pop(0)
            if letter == "H":
                hooks.append([])
            else:
                hooks[-1].append(letter)
        for copy in load_w + ([] if layer == 1 else load_h):
            copy.wait()
        hidden_grads(layer, hooks)
        if layer == 1:
            layer = 0
            load_h = [load(h_hbm.at[0, 0], h_buf, 0)]
            load_w = [load(wd_hbm.at[0], wd_buf, 6), load(wu_hbm.at[0], wu_buf, 7)]


def flush_kernel(g, *refs):
    sums, (g_out, up_out, down_out, sems) = refs[:PARTS], refs[PARTS:]
    copies = []
    for n in range(PARTS):
        layer, half = 1 - n // 4, n % 2
        for q in range(2):
            if n % 4 < 2:
                dst = down_out.at[layer, :, pl.ds(half * F + q * Q, Q)]
            else:
                dst = up_out.at[layer, pl.ds(half * F, F), pl.ds(q * Q, Q)]
            copies.append(pltpu.make_async_copy(sums[n].at[q], dst, sems.at[len(copies)]))
    copies.append(pltpu.make_async_copy(g, g_out.at[0], sems.at[len(copies)]))
    for copy in copies:
        copy.start()
    for copy in copies:
        copy.wait()


def solution(mesh):
    hbm, vmem = pl.BlockSpec(memory_space=pl.ANY), pl.BlockSpec(memory_space=pltpu.VMEM)
    dma, regular = pltpu.SemaphoreType.DMA, pltpu.SemaphoreType.REGULAR

    def run_backward(w_up, w_down, x_saved, h_saved, grad_out):
        results = pl.pallas_call(
            backward_kernel,
            name="backward",
            out_shape=[pltpu.VMEM((T, D), BF16)] + [pltpu.VMEM((2, F, Q), F32)] * PARTS,
            in_specs=[hbm] * 5,
            out_specs=[vmem] * (1 + PARTS),
            scratch_shapes=[
                pltpu.VMEM((T, D), BF16),
                pltpu.VMEM((HALF, D), BF16),
                pltpu.VMEM((T, F), BF16),
                pltpu.VMEM((T, F), BF16),
                pltpu.VMEM((D, F), BF16),
                pltpu.VMEM((F, D), BF16),
                pltpu.VMEM((2, T, 256), BF16),
                pltpu.VMEM((SLOTS, 2, 2, 3, N1, Q), F32),
                pltpu.VMEM((SLOTS, 2, 2, 3, N2, Q), F32),
                pltpu.VMEM((2, 3, TOK // 2, D), BF16),
                dma((SLOTS, 4, 2)),
                dma((SLOTS, 4, 2, 2)),
                regular((PARTS, 2, 2)),
                dma((2, 2)),
                dma((2, 5)),
                regular((2,)),
                dma((2, 5)),
                dma((2, 5)),
                regular((2,)),
                dma((8,)),
                dma((2,)),
            ],
            compiler_params=pltpu.CompilerParams(collective_id=0, has_side_effects=True, vmem_limit_bytes=41800000),
        )(w_up, w_down, x_saved, h_saved, grad_out)
        grad_in, up_total, down_total = pl.pallas_call(
            flush_kernel,
            name="flush",
            out_shape=[jax.ShapeDtypeStruct((1, T, D), BF16), jax.ShapeDtypeStruct((2, D, F), F32), jax.ShapeDtypeStruct((2, F, D), F32)],
            in_specs=[vmem] * (1 + PARTS),
            out_specs=[hbm] * 3,
            scratch_shapes=[dma((2 * PARTS + 1,))],
            compiler_params=pltpu.CompilerParams(vmem_limit_bytes=1 << 20),
        )(*results)
        return grad_in, up_total, down_total

    return jax.shard_map(run_backward, mesh=mesh, in_specs=(P(None, None, "tp"), P(None, "tp", None), P(None, "dp", None, None), P(None, "dp", None, "tp"), P("dp", None, None)), out_specs=(P("dp", None, None), P(None, None, "tp"), P(None, "tp", None)), check_vma=False)
```

```python
import jax
import jax.numpy as jnp
from jax import lax
from jax.experimental import pallas as pl
from jax.experimental.pallas import tpu as pltpu
from jax.sharding import PartitionSpec as P

MESH = pl.DeviceIdType.MESH
F32, BF16 = jnp.float32, jnp.bfloat16
T, D, F = 2048, 1536, 768
HALF = T // 2
TOK = HALF // 4
Q = F // 2
N1, N2 = F // 8, F // 32
PARTS = 8
SLOTS = 4
RS1, RS2, AG2, AG1 = range(4)
DIRS = ((0, 1), (1, -1))

ORDER = (
    "DaDbDcDHdabaHHcbHHdcHadHbHUeacUTfbUdagfbUhdaehegcbhdfTegchab",
    "fehdgcTabfgehddcTfghceacdfTbgTHeheHHhHffbggHheHHaHcgfdDDDkjk",
    "UDllfUngiiTkjilnemmTjlknUmijklUhpoomkjplomkijplTnTmkiojllpnk",
    "opkmlnTpjmonlimjjopmkniTppioinpojomnpion",
)


def gelu_parts(hidden):
    scale = 0.7978845608028654
    square = hidden * hidden
    tanh_val = jnp.tanh(hidden * (scale + (scale * 0.044715) * square))
    upper = 0.5 + 0.5 * tanh_val
    gelu_slope = upper + upper * (1.0 - tanh_val) * hidden * (scale + (scale * 0.134145) * square)
    return hidden * upper, gelu_slope


def backward_kernel(wu_hbm, wd_hbm, x_hbm, h_hbm, g_hbm, buf_a, *refs):
    sums = refs[:PARTS]
    (buf_b, pair_in, h_buf, dh_buf, wu_buf, wd_buf, x_tile, ring1, ring2, xring,
     dp_send, dp_recv, dp_free, x_send, x_recv, x_free, pair_send, pair_recv, pair_free, load_sem, x_sem) = refs[PARTS:]
    dp_pos, tp_pos = lax.axis_index("dp"), lax.axis_index("tp")
    core = lax.rem(tp_pos, 2)
    pos = {"x": tp_pos // 2, "y": lax.rem(dp_pos, 4), "z": dp_pos // 4}
    g_of, p_of = {1: buf_a, 0: buf_b}, {1: buf_b, 0: buf_a}

    def wrap(value):
        return lax.rem(value + 4, 4)

    def neighbour(axis, step):
        moved = wrap(pos[axis] + step)
        if axis == "x":
            return {"dp": dp_pos, "tp": moved * 2 + core}
        if axis == "y":
            return {"dp": pos["z"] * 4 + moved, "tp": tp_pos}
        return {"dp": moved * 4 + pos["y"], "tp": tp_pos}

    partner = {"dp": dp_pos, "tp": pos["x"] * 2 + 1 - core}

    def load(src, dst, k):
        copy = pltpu.make_async_copy(src, dst, load_sem.at[k])
        copy.start()
        return copy

    def x_load(layer, i):
        slot = i % 2
        return pltpu.make_async_copy(x_hbm.at[layer, 0, :, pl.ds(i * Q, Q)], x_tile.at[slot], x_sem.at[slot])

    barrier = pltpu.get_barrier_semaphore()
    for axis in "xyz":
        for _, step in DIRS:
            pl.semaphore_signal(barrier, inc=1, device_id=neighbour(axis, step), device_id_type=MESH)
    pl.semaphore_signal(barrier, inc=1, device_id=partner, device_id_type=MESH)

    load_h, load_g = [], []
    for i in range(2):
        cols = pl.ds(i * Q, Q)
        load_h.append(load(h_hbm.at[1, 0, :, cols], h_buf.at[:, cols], i))
        cols = pl.ds(i * F, F)
        load_g.append(load(g_hbm.at[0, :, cols], buf_a.at[:, cols], 2 + i))
    load_w = [load(wd_hbm.at[1], wd_buf, 4), load(wu_hbm.at[1], wu_buf, 5)]
    x_load(1, 0).start()
    x_load(1, 1).start()

    def remote(src, dst, send_sem, recv_sem, device):
        return pltpu.make_async_remote_copy(src_ref=src, dst_ref=dst, send_sem=send_sem, recv_sem=recv_sem, device_id=device, device_id_type=MESH)

    def dp_axes(stage, colour):
        first, second = ("y", "z") if colour == 0 else ("z", "y")
        return first if stage in (RS1, AG1) else second

    def dp_rows(stage, colour, j):
        if stage in (RS1, AG1):
            return pl.ds(pl.multiple_of(colour * (F // 2) + j * N1, 8), N1)
        return pl.ds(pl.multiple_of(colour * (F // 2) + pos[dp_axes(RS1, colour)] * N1 + j * N2, 8), N2)

    def dp_ring(n, stage, colour):
        return (ring1 if stage in (RS1, AG1) else ring2).at[n % SLOTS, colour]

    def dp_copy(n, stage, colour, di, piece):
        w, axis, step = sums[n], dp_axes(stage, colour), DIRS[di][1]
        p = pos[axis]
        if stage in (RS1, RS2):
            dst = dp_ring(n, stage, colour).at[di, piece]
            if piece == 0:
                src = w.at[di, dp_rows(stage, colour, wrap(p + 2))]
            else:
                src = w.at[1 - di if piece == 1 else di, dp_rows(stage, colour, wrap(p + step))]
        else:
            j = p if piece < 2 else wrap(p - step)
            src = dst = w.at[1 - di if piece == 1 else di, dp_rows(stage, colour, j)]
        return remote(src, dst, dp_send.at[n % SLOTS, stage, colour], dp_recv.at[n % SLOTS, stage, colour, min(piece, 1)], neighbour(axis, step))

    def dp_received(n, stage, colour, last):
        ring = dp_ring(n, stage, colour)
        pieces = ring.at[:, pl.ds(1, 2)] if last else ring.at[:, pl.ds(0, 1)]
        remote(pieces, pieces, dp_send.at[n % SLOTS, stage, colour], dp_recv.at[n % SLOTS, stage, colour, last], partner).wait_recv()

    def dp_sent(n, stage, colour):
        ring = dp_ring(n, stage, colour)
        remote(ring, ring, dp_send.at[n % SLOTS, stage, colour], dp_recv.at[n % SLOTS, stage, colour, 0], partner).wait_send()

    def both(n, stage, colour, piece):
        for di, _ in DIRS:
            dp_copy(n, stage, colour, di, piece).start()

    def rs_mid(n, stage, colour):
        w, axis, ring = sums[n], dp_axes(stage, colour), dp_ring(n, stage, colour)
        dp_received(n, stage, colour, 0)
        for di, step in DIRS:
            near = dp_rows(stage, colour, wrap(pos[axis] + step))
            w[di, near, :] = w[di, near, :] + ring[di, 0]
            dp_copy(n, stage, colour, di, 2).start()

    def rs_end(n, stage, colour):
        w, axis, ring = sums[n], dp_axes(stage, colour), dp_ring(n, stage, colour)
        dp_received(n, stage, colour, 1)
        own = dp_rows(stage, colour, pos[axis])
        for di, _ in DIRS:
            w[di, own, :] = w[di, own, :] + ring[di, 2] + ring[1 - di, 1]

    def rs_free(n, stage, colour):
        dp_sent(n, stage, colour)
        for _, step in DIRS:
            pl.semaphore_signal(dp_free.at[n % SLOTS, stage, colour], inc=1, device_id=neighbour(dp_axes(stage, colour), step), device_id_type=MESH)

    def ag_ready(n, stage, colour):
        pl.semaphore_wait(dp_free.at[n % SLOTS, RS2 if stage == AG2 else RS1, colour], 2)

    def ag_mid(n, stage, colour):
        dp_received(n, stage, colour, 0)
        both(n, stage, colour, 2)

    def dp_step(n, colour, k):
        if k < 2:
            both(n, RS1, colour, k)
        elif k == 2:
            rs_mid(n, RS1, colour)
        elif k == 3:
            rs_end(n, RS1, colour)
            both(n, RS2, colour, 0)
            both(n, RS2, colour, 1)
            rs_free(n, RS1, colour)
        elif k == 4:
            rs_mid(n, RS2, colour)
        elif k == 5:
            rs_end(n, RS2, colour)
            rs_free(n, RS2, colour)
            ag_ready(n, AG2, colour)
            both(n, AG2, colour, 0)
            both(n, AG2, colour, 1)
        elif k == 6:
            ag_mid(n, AG2, colour)
        elif k == 7:
            dp_received(n, AG2, colour, 1)
            ag_ready(n, AG1, colour)
            both(n, AG1, colour, 0)
        elif k == 8:
            both(n, AG1, colour, 1)
        elif k == 9:
            ag_mid(n, AG1, colour)
        else:
            dp_received(n, AG1, colour, 1)
            dp_sent(n, AG2, colour)
            dp_sent(n, AG1, colour)

    def chunk(j, half=None):
        base = core * HALF + j * TOK
        if half is None:
            return pl.ds(pl.multiple_of(base, TOK), TOK)
        return pl.ds(pl.multiple_of(base + half * (TOK // 2), TOK // 2), TOK // 2)

    def x_copy(layer, stage, di, piece):
        p_buf, step, p = p_of[layer], DIRS[di][1], pos["x"]
        if stage == 0:
            dst = xring.at[di, piece]
            src = p_buf.at[chunk(wrap(p + 2), di) if piece == 0 else chunk(wrap(p + step), 1 - di if piece == 1 else di)]
        else:
            src = dst = p_buf.at[chunk(p if piece < 2 else wrap(p - step), 1 - di if piece == 1 else di)]
        recv = min(piece, 1) if stage == 0 else 2 + piece
        return remote(src, dst, x_send.at[stage], x_recv.at[recv], neighbour("x", step))

    def x_received(layer, recv):
        pieces = xring.at[:, pl.ds(1, 2)] if recv == 1 else xring.at[:, pl.ds(0, 1)]
        remote(pieces, pieces, x_send.at[0], x_recv.at[recv], partner).wait_recv()

    def x_sent(layer, stage):
        remote(xring, xring, x_send.at[stage], x_recv.at[0], partner).wait_send()

    def pair_copy(layer, k, src, dst):
        return remote(src, dst, pair_send.at[k], pair_recv.at[k], partner)

    def tp_forward(layer, k):
        part = p_of[layer].at[chunk(wrap(pos["x"] + (0, -1, 1, 2)[k]))]
        return pair_copy(layer, 4, part, part)

    def block(layer, row):
        toks = pl.ds(pl.multiple_of(row, TOK), TOK)
        act_grad = lax.dot_general(g_of[layer][toks, :], wd_buf[...], (((1,), (1,)), ((), ())), preferred_element_type=F32)
        gelu_out, gelu_slope = gelu_parts(h_buf[toks, :].astype(F32))
        hid_grad = (act_grad * gelu_slope).astype(BF16)
        dh_buf[toks, :] = hid_grad
        if layer == 0:
            h_buf[toks, :] = gelu_out.astype(BF16)
        p_of[layer][toks, :] = lax.dot_general(hid_grad, wu_buf[...], (((1,), (1,)), ((), ())), preferred_element_type=F32).astype(BF16)

    def hidden_grads(layer, hooks):
        p_buf = p_of[layer]

        @pl.loop(0, 4)
        def _(i):
            j = lax.rem(pos["x"] + 2 + i, 4)
            other = pl.multiple_of((1 - core) * HALF + j * TOK, TOK)
            block(layer, other)
            landing = pair_in.at[pl.ds(pl.multiple_of(j * TOK, TOK), TOK)]
            copy = pair_copy(layer, i, p_buf.at[pl.ds(other, TOK)], landing)
            copy.start()
            run_hooks(i, hooks[0::2])
            block(layer, pl.multiple_of(core * HALF + j * TOK, TOK))
            copy.wait()
            p_buf[chunk(j), :] = (p_buf[chunk(j), :].astype(F32) + landing[...].astype(F32)).astype(BF16)
            for k in (0, 1, 3):

                @pl.when(i == k)
                def _():
                    if k == 0:
                        x_copy(layer, 0, 0, 0).start()
                        x_copy(layer, 0, 1, 0).start()
                    elif k == 1:
                        x_copy(layer, 0, 1, 1).start()
                    else:
                        x_copy(layer, 0, 0, 1).start()
                        pl.semaphore_signal(pair_free, inc=1, device_id=partner, device_id_type=MESH)

            run_hooks(i, hooks[1::2])

    def run_hooks(i, hooks):
        for k in range(4):
            if hooks[k]:

                @pl.when(i == k)
                def _():
                    for letter in hooks[k]:
                        run(letter)

    def tp_step(layer, k):
        g_buf, p_buf = g_of[layer], p_of[layer]
        if k == 0:
            x_received(layer, 0)
            for di, step in DIRS:
                near = chunk(wrap(pos["x"] + step), di)
                p_buf[near, :] = (p_buf[near, :].astype(F32) + xring[di, 0].astype(F32)).astype(BF16)
                x_copy(layer, 0, di, 2).start()
        elif k == 1:
            x_received(layer, 1)
            x_sent(layer, 0)
            for _, step in DIRS:
                pl.semaphore_signal(x_free, inc=1, device_id=neighbour("x", step), device_id_type=MESH)
            for di, _ in DIRS:
                own = chunk(pos["x"], di)
                total = p_buf[own, :].astype(F32) + xring[di, 2].astype(F32) + xring[1 - di, 1].astype(F32)
                p_buf[own, :] = (g_buf[own, :].astype(F32) + total).astype(BF16)
            pl.semaphore_wait(x_free, 2)
            for piece in range(2):
                for di, _ in DIRS:
                    x_copy(layer, 1, di, piece).start()
            pl.semaphore_wait(pair_free, 1)
            tp_forward(layer, 0).start()
        elif k == 2:
            x_received(layer, 2)
            for di, _ in DIRS:
                x_copy(layer, 1, di, 2).start()
        elif k == 3:
            x_received(layer, 3)
            tp_forward(layer, 1).start()
            tp_forward(layer, 2).start()
        elif k == 4:
            x_received(layer, 4)
            tp_forward(layer, 3).start()
        else:
            pair_copy(layer, 4, pair_in, pair_in).wait()
            x_sent(layer, 1)

    def put(w, at, value):
        w[0, at, :] = value[:, :Q]
        w[1, at, :] = value[:, Q:]

    def down_grad(layer, half, colour):
        gelu_buf, g_buf = (dh_buf, buf_a) if layer == 1 else (h_buf, buf_b)
        cols = pl.ds(colour * Q, Q)
        if layer == 1 and half == 0:
            load_h[colour].wait()

            @pl.loop(0, T // 256)
            def _(i):
                toks = pl.ds(pl.multiple_of(i * 256, 256), 256)
                dh_buf[toks, cols] = gelu_parts(h_buf[toks, cols].astype(F32))[0].astype(BF16)

        if layer == 1 and colour == 0:
            load_g[half].wait()
        put(sums[(1 - layer) * 4 + half], cols,
            lax.dot_general(gelu_buf[:, cols], g_buf[:, half * F:(half + 1) * F], (((0,), (0,)), ((), ())), preferred_element_type=F32))

    def up_grad(layer, half, colour):
        i = half * 2 + colour
        x_load(layer, i).wait()
        put(sums[(1 - layer) * 4 + 2 + half], pl.ds(colour * Q, Q),
            lax.dot_general(x_tile[i % 2], dh_buf[...], (((0,), (0,)), ((), ())), preferred_element_type=F32))
        if i < 2:
            x_load(layer, i + 2).start()
        elif layer == 1:
            x_load(0, i - 2).start()

    taken = {}

    def run(letter):
        count = taken[letter] = taken.get(letter, -1) + 1
        if letter == "D":
            down_grad(1 - count // 4, count // 2 % 2, count % 2)
        elif letter == "U":
            up_grad(1 - count // 4, count // 2 % 2, count % 2)
        elif letter == "T":
            tp_step(1 - count // 6, count % 6)
        else:
            part = ord(letter) - ord("a")
            dp_step(part // 2, part % 2, count)

    todo = list("".join(ORDER))
    layer = 1
    run(todo.pop(0))
    pl.semaphore_wait(barrier, 7)
    while todo:
        if todo[0] != "H":
            run(todo.pop(0))
            continue
        hooks = []
        while len(hooks) < 8:
            letter = todo.pop(0)
            if letter == "H":
                hooks.append([])
            else:
                hooks[-1].append(letter)
        for copy in load_w + ([] if layer == 1 else load_h):
            copy.wait()
        hidden_grads(layer, hooks)
        if layer == 1:
            layer = 0
            load_h = [load(h_hbm.at[0, 0], h_buf, 0)]
            load_w = [load(wd_hbm.at[0], wd_buf, 4), load(wu_hbm.at[0], wu_buf, 5)]


def flush_kernel(g, *refs):
    sums, (g_out, up_out, down_out, sems) = refs[:PARTS], refs[PARTS:]
    copies = []
    for n in range(PARTS):
        layer, half = 1 - n // 4, n % 2
        for q in range(2):
            if n % 4 < 2:
                dst = down_out.at[layer, :, pl.ds(half * F + q * Q, Q)]
            else:
                dst = up_out.at[layer, pl.ds(half * F, F), pl.ds(q * Q, Q)]
            copies.append(pltpu.make_async_copy(sums[n].at[q], dst, sems.at[len(copies)]))
    copies.append(pltpu.make_async_copy(g, g_out.at[0], sems.at[len(copies)]))
    for copy in copies:
        copy.start()
    for copy in copies:
        copy.wait()


def solution(mesh):
    hbm, vmem = pl.BlockSpec(memory_space=pl.ANY), pl.BlockSpec(memory_space=pltpu.VMEM)
    dma, regular = pltpu.SemaphoreType.DMA, pltpu.SemaphoreType.REGULAR

    def run_backward(w_up, w_down, x_saved, h_saved, grad_out):
        results = pl.pallas_call(
            backward_kernel,
            name="backward",
            out_shape=[pltpu.VMEM((T, D), BF16)] + [pltpu.VMEM((2, F, Q), F32)] * PARTS,
            in_specs=[hbm] * 5,
            out_specs=[vmem] * (1 + PARTS),
            scratch_shapes=[
                pltpu.VMEM((T, D), BF16),
                pltpu.VMEM((HALF, D), BF16),
                pltpu.VMEM((T, F), BF16),
                pltpu.VMEM((T, F), BF16),
                pltpu.VMEM((D, F), BF16),
                pltpu.VMEM((F, D), BF16),
                pltpu.VMEM((2, T, Q), BF16),
                pltpu.VMEM((SLOTS, 2, 2, 3, N1, Q), F32),
                pltpu.VMEM((SLOTS, 2, 2, 3, N2, Q), F32),
                pltpu.VMEM((2, 3, TOK // 2, D), BF16),
                dma((SLOTS, 4, 2)),
                dma((SLOTS, 4, 2, 2)),
                regular((SLOTS, 2, 2)),
                dma((2,)),
                dma((5,)),
                regular,
                dma((5,)),
                dma((5,)),
                regular,
                dma((6,)),
                dma((2,)),
            ],
            compiler_params=pltpu.CompilerParams(collective_id=0, has_side_effects=True, vmem_limit_bytes=41800000),
        )(w_up, w_down, x_saved, h_saved, grad_out)
        grad_in, up_total, down_total = pl.pallas_call(
            flush_kernel,
            name="flush",
            out_shape=[jax.ShapeDtypeStruct((1, T, D), BF16), jax.ShapeDtypeStruct((2, D, F), F32), jax.ShapeDtypeStruct((2, F, D), F32)],
            in_specs=[vmem] * (1 + PARTS),
            out_specs=[hbm] * 3,
            scratch_shapes=[dma((2 * PARTS + 1,))],
            compiler_params=pltpu.CompilerParams(vmem_limit_bytes=1 << 20),
        )(*results)
        return grad_in, up_total, down_total

    return jax.shard_map(run_backward, mesh=mesh, in_specs=(P(None, None, "tp"), P(None, "tp", None), P(None, "dp", None, None), P(None, "dp", None, "tp"), P("dp", None, None)), out_specs=(P("dp", None, None), P(None, None, "tp"), P(None, "tp", None)), check_vma=False)
```

```python
import jax
import jax.numpy as jnp
from jax import lax
from jax.experimental import pallas as pl
from jax.experimental.pallas import tpu as pltpu
from jax.sharding import PartitionSpec as P

MESH = pl.DeviceIdType.MESH
F32, BF16 = jnp.float32, jnp.bfloat16
T, D, F = 2048, 1536, 768
HALF = T // 2
TOK = HALF // 4
Q = F // 2
N1, N2 = F // 8, F // 32
PARTS = 8
SLOTS = 4
RS1, RS2, AG2, AG1 = range(4)
DIRS = ((0, 1), (1, -1))

ORDER = (
    "DaDbDcDHdabaHHcbHHdcHadHbHUeacUTfbUdagfbUhdaehegcbhdfTegchab",
    "fehdgcTabfgehddcTfghceacdfTbgTHeheHHhHffbggHheHHaHcgfdDDDkjk",
    "UDllfUngiiTkjilnemmTjlknUmijklUhpoomkjplomkijplTnTmkiojllpnk",
    "opkmlnTpjmonlimjjopmkniTppioinpojomnpion",
)


def gelu_parts(hidden):
    scale = 0.7978845608028654
    eighth = hidden * (0.125 * hidden)
    tanh_val = jnp.tanh(hidden * (scale + (scale * 0.35772) * eighth))
    upper = 0.5 + 0.5 * tanh_val
    gelu_slope = upper + upper * (1.0 - tanh_val) * hidden * (scale + (scale * 1.07316) * eighth)
    return hidden * upper, gelu_slope


def backward_kernel(wu_hbm, wd_hbm, x_hbm, h_hbm, g_hbm, buf_a, *refs):
    sums = refs[:PARTS]
    (buf_b, pair_in, h_buf, dh_buf, wu_buf, wd_buf, x_tile, ring1, ring2, xring,
     dp_send, dp_recv, dp_free, x_send, x_recv, x_free, pair_send, pair_recv, pair_free, load_sem, x_sem) = refs[PARTS:]
    dp_pos, tp_pos = lax.axis_index("dp"), lax.axis_index("tp")
    core = lax.rem(tp_pos, 2)
    pos = {"x": tp_pos // 2, "y": lax.rem(dp_pos, 4), "z": dp_pos // 4}
    g_of, p_of = {1: buf_a, 0: buf_b}, {1: buf_b, 0: buf_a}

    def wrap(value):
        return lax.rem(value + 4, 4)

    def neighbour(axis, step):
        moved = wrap(pos[axis] + step)
        if axis == "x":
            return {"dp": dp_pos, "tp": moved * 2 + core}
        if axis == "y":
            return {"dp": pos["z"] * 4 + moved, "tp": tp_pos}
        return {"dp": moved * 4 + pos["y"], "tp": tp_pos}

    partner = {"dp": dp_pos, "tp": pos["x"] * 2 + 1 - core}

    def load(src, dst, k):
        copy = pltpu.make_async_copy(src, dst, load_sem.at[k])
        copy.start()
        return copy

    def x_load(layer, i):
        slot = i % 2
        return pltpu.make_async_copy(x_hbm.at[layer, 0, :, pl.ds(i * Q, Q)], x_tile.at[slot], x_sem.at[slot])

    load_h, load_g = [], []
    for i in range(2):
        cols = pl.ds(i * Q, Q)
        load_h.append(load(h_hbm.at[1, 0, :, cols], h_buf.at[:, cols], i))
        cols = pl.ds(i * F, F)
        load_g.append(load(g_hbm.at[0, :, cols], buf_a.at[:, cols], 2 + i))
    load_w = [load(wd_hbm.at[1], wd_buf, 4), load(wu_hbm.at[1], wu_buf, 5)]
    x_load(1, 0).start()
    x_load(1, 1).start()

    barrier = pltpu.get_barrier_semaphore()
    for axis in "xyz":
        for _, step in DIRS:
            pl.semaphore_signal(barrier, inc=1, device_id=neighbour(axis, step), device_id_type=MESH)
    pl.semaphore_signal(barrier, inc=1, device_id=partner, device_id_type=MESH)

    def remote(src, dst, send_sem, recv_sem, device):
        return pltpu.make_async_remote_copy(src_ref=src, dst_ref=dst, send_sem=send_sem, recv_sem=recv_sem, device_id=device, device_id_type=MESH)

    def dp_axes(stage, colour):
        first, second = ("y", "z") if colour == 0 else ("z", "y")
        return first if stage in (RS1, AG1) else second

    def dp_rows(stage, colour, j):
        if stage in (RS1, AG1):
            return pl.ds(pl.multiple_of(colour * (F // 2) + j * N1, 8), N1)
        return pl.ds(pl.multiple_of(colour * (F // 2) + pos[dp_axes(RS1, colour)] * N1 + j * N2, 8), N2)

    def dp_ring(n, stage, colour):
        return (ring1 if stage in (RS1, AG1) else ring2).at[n % SLOTS, colour]

    def dp_copy(n, stage, colour, di, piece):
        w, axis, step = sums[n], dp_axes(stage, colour), DIRS[di][1]
        p = pos[axis]
        if stage in (RS1, RS2):
            dst = dp_ring(n, stage, colour).at[di, piece]
            if piece == 0:
                src = w.at[di, dp_rows(stage, colour, wrap(p + 2))]
            else:
                src = w.at[1 - di if piece == 1 else di, dp_rows(stage, colour, wrap(p + step))]
        else:
            j = p if piece < 2 else wrap(p - step)
            src = dst = w.at[1 - di if piece == 1 else di, dp_rows(stage, colour, j)]
        return remote(src, dst, dp_send.at[n % SLOTS, stage, colour], dp_recv.at[n % SLOTS, stage, colour, min(piece, 1)], neighbour(axis, step))

    def dp_received(n, stage, colour, last):
        ring = dp_ring(n, stage, colour)
        pieces = ring.at[:, pl.ds(1, 2)] if last else ring.at[:, pl.ds(0, 1)]
        remote(pieces, pieces, dp_send.at[n % SLOTS, stage, colour], dp_recv.at[n % SLOTS, stage, colour, last], partner).wait_recv()

    def dp_sent(n, stage, colour):
        ring = dp_ring(n, stage, colour)
        remote(ring, ring, dp_send.at[n % SLOTS, stage, colour], dp_recv.at[n % SLOTS, stage, colour, 0], partner).wait_send()

    def both(n, stage, colour, piece):
        for di, _ in DIRS:
            dp_copy(n, stage, colour, di, piece).start()

    def rs_mid(n, stage, colour):
        w, axis, ring = sums[n], dp_axes(stage, colour), dp_ring(n, stage, colour)
        dp_received(n, stage, colour, 0)
        for di, step in DIRS:
            near = dp_rows(stage, colour, wrap(pos[axis] + step))
            w[di, near, :] = w[di, near, :] + ring[di, 0]
            dp_copy(n, stage, colour, di, 2).start()

    def rs_end(n, stage, colour):
        w, axis, ring = sums[n], dp_axes(stage, colour), dp_ring(n, stage, colour)
        dp_received(n, stage, colour, 1)
        own = dp_rows(stage, colour, pos[axis])
        for di, _ in DIRS:
            w[di, own, :] = w[di, own, :] + ring[di, 2] + ring[1 - di, 1]

    def rs_free(n, stage, colour):
        dp_sent(n, stage, colour)
        for _, step in DIRS:
            pl.semaphore_signal(dp_free.at[n % SLOTS, stage, colour], inc=1, device_id=neighbour(dp_axes(stage, colour), step), device_id_type=MESH)

    def ag_ready(n, stage, colour):
        pl.semaphore_wait(dp_free.at[n % SLOTS, RS2 if stage == AG2 else RS1, colour], 2)

    def ag_mid(n, stage, colour):
        dp_received(n, stage, colour, 0)
        both(n, stage, colour, 2)

    def dp_step(n, colour, k):
        if k < 2:
            both(n, RS1, colour, k)
        elif k == 2:
            rs_mid(n, RS1, colour)
        elif k == 3:
            rs_end(n, RS1, colour)
            both(n, RS2, colour, 0)
            both(n, RS2, colour, 1)
            rs_free(n, RS1, colour)
        elif k == 4:
            rs_mid(n, RS2, colour)
        elif k == 5:
            rs_end(n, RS2, colour)
            rs_free(n, RS2, colour)
            ag_ready(n, AG2, colour)
            both(n, AG2, colour, 0)
            both(n, AG2, colour, 1)
        elif k == 6:
            ag_mid(n, AG2, colour)
        elif k == 7:
            dp_received(n, AG2, colour, 1)
            ag_ready(n, AG1, colour)
            both(n, AG1, colour, 0)
        elif k == 8:
            both(n, AG1, colour, 1)
        elif k == 9:
            ag_mid(n, AG1, colour)
        else:
            dp_received(n, AG1, colour, 1)
            dp_sent(n, AG2, colour)
            dp_sent(n, AG1, colour)

    def chunk(j, half=None):
        base = core * HALF + j * TOK
        if half is None:
            return pl.ds(pl.multiple_of(base, TOK), TOK)
        return pl.ds(pl.multiple_of(base + half * (TOK // 2), TOK // 2), TOK // 2)

    def x_copy(layer, stage, di, piece):
        p_buf, step, p = p_of[layer], DIRS[di][1], pos["x"]
        if stage == 0:
            dst = xring.at[di, piece]
            src = p_buf.at[chunk(wrap(p + 2), di) if piece == 0 else chunk(wrap(p + step), 1 - di if piece == 1 else di)]
        else:
            src = dst = p_buf.at[chunk(p if piece < 2 else wrap(p - step), 1 - di if piece == 1 else di)]
        recv = min(piece, 1) if stage == 0 else 2 + piece
        return remote(src, dst, x_send.at[stage], x_recv.at[recv], neighbour("x", step))

    def x_received(layer, recv):
        pieces = xring.at[:, pl.ds(1, 2)] if recv == 1 else xring.at[:, pl.ds(0, 1)]
        remote(pieces, pieces, x_send.at[0], x_recv.at[recv], partner).wait_recv()

    def x_sent(layer, stage):
        remote(xring, xring, x_send.at[stage], x_recv.at[0], partner).wait_send()

    def pair_copy(layer, k, src, dst):
        return remote(src, dst, pair_send.at[k], pair_recv.at[k], partner)

    def tp_forward(layer, k):
        part = p_of[layer].at[chunk(wrap(pos["x"] + (0, -1, 1, 2)[k]))]
        return pair_copy(layer, 4, part, part)

    def block(layer, row):
        toks = pl.ds(pl.multiple_of(row, TOK), TOK)
        act_grad = lax.dot_general(g_of[layer][toks, :], wd_buf[...], (((1,), (1,)), ((), ())), preferred_element_type=F32)
        gelu_out, gelu_slope = gelu_parts(h_buf[toks, :].astype(F32))
        hid_grad = (act_grad * gelu_slope).astype(BF16)
        dh_buf[toks, :] = hid_grad
        if layer == 0:
            h_buf[toks, :] = gelu_out.astype(BF16)
        p_of[layer][toks, :] = lax.dot_general(hid_grad, wu_buf[...], (((1,), (1,)), ((), ())), preferred_element_type=F32).astype(BF16)

    def hidden_grads(layer, hooks):
        p_buf = p_of[layer]

        @pl.loop(0, 4)
        def _(i):
            j = lax.rem(pos["x"] + 2 + i, 4)
            other = pl.multiple_of((1 - core) * HALF + j * TOK, TOK)
            block(layer, other)
            landing = pair_in.at[pl.ds(pl.multiple_of(j * TOK, TOK), TOK)]
            copy = pair_copy(layer, i, p_buf.at[pl.ds(other, TOK)], landing)
            copy.start()
            run_hooks(i, hooks[0::2])
            block(layer, pl.multiple_of(core * HALF + j * TOK, TOK))
            copy.wait()
            p_buf[chunk(j), :] = (p_buf[chunk(j), :].astype(F32) + landing[...].astype(F32)).astype(BF16)
            for k in (0, 1, 3):

                @pl.when(i == k)
                def _():
                    if k == 0:
                        x_copy(layer, 0, 0, 0).start()
                        x_copy(layer, 0, 1, 0).start()
                    elif k == 1:
                        x_copy(layer, 0, 1, 1).start()
                    else:
                        x_copy(layer, 0, 0, 1).start()
                        pl.semaphore_signal(pair_free, inc=1, device_id=partner, device_id_type=MESH)

            run_hooks(i, hooks[1::2])

    def run_hooks(i, hooks):
        for k in range(4):
            if hooks[k]:

                @pl.when(i == k)
                def _():
                    for letter in hooks[k]:
                        run(letter)

    def tp_step(layer, k):
        g_buf, p_buf = g_of[layer], p_of[layer]
        if k == 0:
            x_received(layer, 0)
            for di, step in DIRS:
                near = chunk(wrap(pos["x"] + step), di)
                p_buf[near, :] = (p_buf[near, :].astype(F32) + xring[di, 0].astype(F32)).astype(BF16)
                x_copy(layer, 0, di, 2).start()
        elif k == 1:
            x_received(layer, 1)
            x_sent(layer, 0)
            for _, step in DIRS:
                pl.semaphore_signal(x_free, inc=1, device_id=neighbour("x", step), device_id_type=MESH)
            for di, _ in DIRS:
                own = chunk(pos["x"], di)
                total = p_buf[own, :].astype(F32) + xring[di, 2].astype(F32) + xring[1 - di, 1].astype(F32)
                p_buf[own, :] = (g_buf[own, :].astype(F32) + total).astype(BF16)
            pl.semaphore_wait(x_free, 2)
            for piece in range(2):
                for di, _ in DIRS:
                    x_copy(layer, 1, di, piece).start()
            pl.semaphore_wait(pair_free, 1)
            tp_forward(layer, 0).start()
        elif k == 2:
            x_received(layer, 2)
            for di, _ in DIRS:
                x_copy(layer, 1, di, 2).start()
        elif k == 3:
            x_received(layer, 3)
            tp_forward(layer, 1).start()
            tp_forward(layer, 2).start()
        elif k == 4:
            x_received(layer, 4)
            tp_forward(layer, 3).start()
        else:
            pair_copy(layer, 4, pair_in, pair_in).wait()
            x_sent(layer, 1)

    def put(w, at, value):
        w[0, at, :] = value[:, :Q]
        w[1, at, :] = value[:, Q:]

    def down_grad(layer, half, colour):
        gelu_buf, g_buf = (dh_buf, buf_a) if layer == 1 else (h_buf, buf_b)
        cols = pl.ds(colour * Q, Q)
        if layer == 1 and half == 0:
            load_h[colour].wait()

            @pl.loop(0, T // 256)
            def _(i):
                toks = pl.ds(pl.multiple_of(i * 256, 256), 256)
                dh_buf[toks, cols] = gelu_parts(h_buf[toks, cols].astype(F32))[0].astype(BF16)

        if layer == 1 and colour == 0:
            load_g[half].wait()
        put(sums[(1 - layer) * 4 + half], cols,
            lax.dot_general(gelu_buf[:, cols], g_buf[:, half * F:(half + 1) * F], (((0,), (0,)), ((), ())), preferred_element_type=F32))

    def up_grad(layer, half, colour):
        i = half * 2 + colour
        x_load(layer, i).wait()
        put(sums[(1 - layer) * 4 + 2 + half], pl.ds(colour * Q, Q),
            lax.dot_general(x_tile[i % 2], dh_buf[...], (((0,), (0,)), ((), ())), preferred_element_type=F32))
        if i < 2:
            x_load(layer, i + 2).start()
        elif layer == 1:
            x_load(0, i - 2).start()

    taken = {}

    def run(letter):
        count = taken[letter] = taken.get(letter, -1) + 1
        if letter == "D":
            down_grad(1 - count // 4, count // 2 % 2, count % 2)
        elif letter == "U":
            up_grad(1 - count // 4, count // 2 % 2, count % 2)
        elif letter == "T":
            tp_step(1 - count // 6, count % 6)
        else:
            part = ord(letter) - ord("a")
            dp_step(part // 2, part % 2, count)

    todo = list("".join(ORDER))
    layer = 1
    run(todo.pop(0))
    pl.semaphore_wait(barrier, 7)
    while todo:
        if todo[0] != "H":
            run(todo.pop(0))
            continue
        hooks = []
        while len(hooks) < 8:
            letter = todo.pop(0)
            if letter == "H":
                hooks.append([])
            else:
                hooks[-1].append(letter)
        for copy in load_w + ([] if layer == 1 else load_h):
            copy.wait()
        hidden_grads(layer, hooks)
        if layer == 1:
            layer = 0
            load_h = [load(h_hbm.at[0, 0], h_buf, 0)]
            load_w = [load(wd_hbm.at[0], wd_buf, 4), load(wu_hbm.at[0], wu_buf, 5)]


def flush_kernel(g, *refs):
    sums, (g_out, up_out, down_out, sems) = refs[:PARTS], refs[PARTS:]
    copies = []
    for n in range(PARTS):
        layer, half = 1 - n // 4, n % 2
        for q in range(2):
            if n % 4 < 2:
                dst = down_out.at[layer, :, pl.ds(half * F + q * Q, Q)]
            else:
                dst = up_out.at[layer, pl.ds(half * F, F), pl.ds(q * Q, Q)]
            copies.append(pltpu.make_async_copy(sums[n].at[q], dst, sems.at[len(copies)]))
    copies.append(pltpu.make_async_copy(g, g_out.at[0], sems.at[len(copies)]))
    for copy in copies:
        copy.start()
    for copy in copies:
        copy.wait()


def solution(mesh):
    hbm, vmem = pl.BlockSpec(memory_space=pl.ANY), pl.BlockSpec(memory_space=pltpu.VMEM)
    dma, regular = pltpu.SemaphoreType.DMA, pltpu.SemaphoreType.REGULAR

    def run_backward(w_up, w_down, x_saved, h_saved, grad_out):
        results = pl.pallas_call(
            backward_kernel,
            name="backward",
            out_shape=[pltpu.VMEM((T, D), BF16)] + [pltpu.VMEM((2, F, Q), F32)] * PARTS,
            in_specs=[hbm] * 5,
            out_specs=[vmem] * (1 + PARTS),
            scratch_shapes=[
                pltpu.VMEM((T, D), BF16),
                pltpu.VMEM((HALF, D), BF16),
                pltpu.VMEM((T, F), BF16),
                pltpu.VMEM((T, F), BF16),
                pltpu.VMEM((D, F), BF16),
                pltpu.VMEM((F, D), BF16),
                pltpu.VMEM((2, T, Q), BF16),
                pltpu.VMEM((SLOTS, 2, 2, 3, N1, Q), F32),
                pltpu.VMEM((SLOTS, 2, 2, 3, N2, Q), F32),
                pltpu.VMEM((2, 3, TOK // 2, D), BF16),
                dma((SLOTS, 4, 2)),
                dma((SLOTS, 4, 2, 2)),
                regular((SLOTS, 2, 2)),
                dma((2,)),
                dma((5,)),
                regular,
                dma((5,)),
                dma((5,)),
                regular,
                dma((6,)),
                dma((2,)),
            ],
            compiler_params=pltpu.CompilerParams(collective_id=0, has_side_effects=True, vmem_limit_bytes=41800000),
        )(w_up, w_down, x_saved, h_saved, grad_out)
        grad_in, up_total, down_total = pl.pallas_call(
            flush_kernel,
            name="flush",
            out_shape=[jax.ShapeDtypeStruct((1, T, D), BF16), jax.ShapeDtypeStruct((2, D, F), F32), jax.ShapeDtypeStruct((2, F, D), F32)],
            in_specs=[vmem] * (1 + PARTS),
            out_specs=[hbm] * 3,
            scratch_shapes=[dma((2 * PARTS + 1,))],
            compiler_params=pltpu.CompilerParams(vmem_limit_bytes=1 << 20),
        )(*results)
        return grad_in, up_total, down_total

    return jax.shard_map(run_backward, mesh=mesh, in_specs=(P(None, None, "tp"), P(None, "tp", None), P(None, "dp", None, None), P(None, "dp", None, "tp"), P("dp", None, None)), out_specs=(P("dp", None, None), P(None, None, "tp"), P(None, "tp", None)), check_vma=False)
```
